32 devices in a mesh: seq: 8 (over z, y), head: 4 (over x, core).
Axes of the slice: x: 2, y: 2, z: 4, core: 2. Of those that a mesh axis runs over, the one named last changes fastest.
Arguments:
- query_rows: bfloat16 [8192, 4096], P('seq', 'head'), may hold values from -6 to 6
- key_rows: bfloat16 [8192, 4096], P('seq', 'head'), may hold values from -6 to 6
- value_rows: bfloat16 [8192, 4096], P('seq', 'head'), may hold values from -15 to 15
- block_picks: int32 [16, 32, 4], P('seq', 'head'), may hold values from -1 to 15, as said below
- out_weight: bfloat16 [4096, 4096], P(None, 'head'), may hold values from -0.09375 to 0.09375
Outputs:
- mixed: bfloat16 [8192, 4096], P('seq', 'head')
The draws below stay inside these ranges and needn't reach their ends.
Inputs may be any that keep to these rules, and one draw needn't show every extreme that they name: `block_picks`: every entry that is not -1 names a block held by a lower index of seq than block b. Repeated entries of one row count once. Over the query blocks of one index of seq and the heads of one index of head, at most 2 entries name blocks of any one other index of seq, and every index of seq from 1 on has exactly 2 entries naming blocks of index 0.
All inputs are finite; a program needn't handle non-finite values.
Results may differ from the reference program's by a relative error of at most 0.0059.
Values may be sent and summed in bfloat16 or wider, within the bound.
A program may use at most 192 MiB of HBM per device.

```python
import jax
import jax.numpy as jnp
import numpy as np
from jax import lax

HEADS = 32
HEAD_DIM = 128
D = 4096
BLOCK = 512
TOPK = 5
CAP = 2
BLK_DEV = 2
SEQ = 8192
N_SEQ = 8
N_HEAD = 4


def drawn_pair(key):
    row_count = BLK_DEV * BLOCK * N_SEQ
    width_all = HEADS * HEAD_DIM
    streams = jax.random.split(jax.random.fold_in(key, 7001), 2)
    queries = jnp.clip(1.5 * jax.random.normal(streams[0], (row_count, width_all), jnp.float32), -6.0, 6.0)
    keys_drawn = jnp.clip(1.5 * jax.random.normal(streams[1], (row_count, width_all), jnp.float32), -6.0, 6.0)
    return (queries, keys_drawn)


def draw_query_rows(key, part):
    return drawn_pair(key)[0].astype(jnp.bfloat16)


def draw_key_rows(key, part):
    return drawn_pair(key)[1].astype(jnp.bfloat16)


def draw_block_picks(key, part):
    group_heads = HEADS // N_HEAD
    pair_count = BLK_DEV * group_heads
    slot_count = TOPK - 1
    entry_count = pair_count * slot_count
    seat_count = (N_SEQ - 1) * CAP
    later_count = entry_count - CAP
    later_entries = jnp.asarray(np.array([index_value for index_value in range(entry_count) if index_value % slot_count != 0], dtype=np.int32))

    def one_list(group_id, requester):
        list_key = jax.random.fold_in(jax.random.fold_in(key, 9103), group_id * N_SEQ + requester)
        streams = jax.random.split(list_key, 4)
        first_entries = jax.random.permutation(streams[0], pair_count).astype(jnp.int32) * slot_count
        later_order = jax.random.permutation(streams[1], later_entries).astype(jnp.int32)
        order_list = jnp.concatenate([first_entries, later_order])
        seat_perm = jax.random.permutation(streams[2], seat_count).astype(jnp.int32)
        seat_owner = seat_perm // CAP + 1
        blocked = (seat_owner >= requester).astype(jnp.int32)
        ranked = jnp.argsort(blocked * seat_count + jnp.arange(seat_count, dtype=jnp.int32))
        usable_count = jnp.sum(1 - blocked)
        sorted_owner = jnp.concatenate([seat_owner[ranked], jnp.full((later_count,), -1, jnp.int32)])
        position = jnp.arange(later_count, dtype=jnp.int32)
        later_owner = jnp.where(position < usable_count, sorted_owner[position], -1)
        hot_owner = jnp.where(requester >= 1, jnp.zeros((CAP,), jnp.int32), -1)
        owners = jnp.concatenate([hot_owner, later_owner])
        within = jax.random.randint(streams[3], (entry_count,), 0, BLK_DEV).astype(jnp.int32)
        chosen = jnp.where(owners >= 0, owners * BLK_DEV + within, -1)
        listed = jnp.zeros((entry_count,), jnp.int32).at[order_list].set(chosen)
        return listed.reshape(BLK_DEV, group_heads, slot_count)
    requesters = jnp.arange(N_SEQ, dtype=jnp.int32)
    all_lists = jax.vmap(lambda group_id: jax.vmap(lambda requester: one_list(group_id, requester))(requesters))(jnp.arange(N_HEAD, dtype=jnp.int32))
    all_lists = jnp.transpose(all_lists, (1, 2, 0, 3, 4))
    return all_lists.reshape(N_SEQ * BLK_DEV, HEADS, slot_count)


def block_scale(stream_key, extent, pieces, smallest, high):
    def one(axis_at, shards_of):
        draws = jax.random.uniform(jax.random.fold_in(jax.random.fold_in(stream_key, 6), axis_at), (shards_of,), jnp.float32, smallest / len(pieces), high / len(pieces))
        return jnp.repeat(jnp.exp(draws), extent[axis_at] // shards_of).reshape((-1,) + (1,) * (len(extent) - axis_at - 1))

    factor_of = one(*pieces[0])
    for cut in pieces[1:]:
        factor_of = factor_of * one(*cut)
    return factor_of


def gaussian(rng, dims, deviation, bound, shards=(), held_as=jnp.bfloat16):
    drawn = deviation * jax.random.normal(rng, dims, jnp.float32)
    if shards:
        drawn = drawn * block_scale(rng, dims, shards, -0.22, 0.18)
    return jnp.clip(drawn, -bound, bound).astype(held_as)


def setup_inputs(seed: int = 0) -> dict:
    key_of = jax.random.split(jax.random.key(seed), 6)
    query_rows = draw_query_rows(jax.random.fold_in(key_of[5], 71), 0)
    key_rows = draw_key_rows(jax.random.fold_in(key_of[5], 71), 0)
    value_rows = gaussian(key_of[2], (SEQ, HEADS * HEAD_DIM), 3.0, 15.0, ((0, 8), (1, 4)))
    block_picks = draw_block_picks(jax.random.fold_in(key_of[5], 71), 0)
    out_weight = gaussian(key_of[4], (HEADS * HEAD_DIM, D), (HEADS * HEAD_DIM) ** -0.5, 0.09375, ((1, 4),))
    return {"query_rows": query_rows, "key_rows": key_rows, "value_rows": value_rows, "block_picks": block_picks, "out_weight": out_weight}


def block_partial(query_tile, key_tile, value_tile, causal_mask):
    score_scale = HEAD_DIM ** -0.5
    scores = jnp.einsum("hqd,hkd->hqk", query_tile.astype(jnp.float32), key_tile.astype(jnp.float32)) * score_scale
    if causal_mask is not None:
        scores = jnp.where(causal_mask, scores, -jnp.inf)
    maxima = jnp.max(scores, axis=-1)
    shifted = jnp.exp(scores - maxima[..., None])
    totals = jnp.sum(shifted, axis=-1)
    weights = shifted.astype(jnp.bfloat16)
    partial_out = jnp.einsum("hqk,hkd->hqd", weights.astype(jnp.float32), value_tile.astype(jnp.float32))
    return partial_out.astype(jnp.bfloat16), maxima, totals


def merge_parts(outputs, maxima, totals, usable):
    keep = usable[:, :, None]
    largest = jnp.max(jnp.where(keep, maxima, -jnp.inf), axis=0)
    factor = jnp.where(keep, jnp.exp(maxima - largest[None]), 0.0)
    numer = jnp.sum(factor[..., None] * outputs.astype(jnp.float32), axis=0)
    denom = jnp.sum(factor * totals, axis=0)
    return (numer / denom[..., None]).astype(jnp.bfloat16)


def reference(query_rows, key_rows, value_rows, block_picks, out_weight):
    block_count = query_rows.shape[0] // BLOCK
    block_shape = (block_count, BLOCK, HEADS, HEAD_DIM)
    queries = query_rows.reshape(block_shape)
    key_blocks = key_rows.reshape(block_shape)
    value_blocks = value_rows.reshape(block_shape)
    positions = jnp.arange(BLOCK)
    causal_mask = positions[:, None] >= positions[None, :]
    head_index = jnp.arange(HEADS)

    def one_block(block_id):
        query_tile = jnp.transpose(queries[block_id], (1, 0, 2))
        own_part = block_partial(query_tile, jnp.transpose(key_blocks[block_id], (1, 0, 2)),
                                 jnp.transpose(value_blocks[block_id], (1, 0, 2)), causal_mask)
        chosen = block_picks[block_id]
        part_outputs = [own_part[0]]
        part_maxima = [own_part[1]]
        part_totals = [own_part[2]]
        part_usable = [jnp.ones((HEADS,), dtype=jnp.bool_)]
        for column in range(chosen.shape[1]):
            entries = chosen[:, column]
            usable = entries >= 0
            for earlier in range(column):
                usable = usable & (entries != chosen[:, earlier])
            safe_index = jnp.where(usable, entries, 0)
            result_part = block_partial(query_tile, key_blocks[safe_index, :, head_index, :],
                                        value_blocks[safe_index, :, head_index, :], None)
            part_outputs.append(result_part[0])
            part_maxima.append(result_part[1])
            part_totals.append(result_part[2])
            part_usable.append(usable)
        combined = merge_parts(jnp.stack(part_outputs), jnp.stack(part_maxima), jnp.stack(part_totals),
                               jnp.stack(part_usable))
        return jnp.transpose(combined, (1, 0, 2)).reshape(BLOCK, HEADS * HEAD_DIM)

    attended = lax.map(one_block, jnp.arange(block_count, dtype=jnp.int32)).reshape(-1, HEADS * HEAD_DIM)
    return jnp.dot(attended, out_weight, preferred_element_type=jnp.float32).astype(jnp.bfloat16)
```

```python
import functools
import math

import jax
import jax.numpy as jnp
from jax import lax
from jax.experimental import pallas as pl
from jax.experimental.pallas import tpu as pltpu
from jax.sharding import PartitionSpec as P

CAP = 2
MESH = pl.DeviceIdType.MESH
F32 = jnp.float32
BF16 = jnp.bfloat16


def loop(lower, upper, step):
    def body(i, carry):
        step(i)
        return carry

    lax.fori_loop(lower, upper, body, 0)


def attend(query, key, value, causal_start=None):
    scale = query.shape[-1] ** -0.5
    scores = lax.dot_general(
        key, query, (((1,), (1,)), ((), ())), preferred_element_type=F32
    )
    if causal_start is not None:
        key_at = lax.broadcasted_iota(jnp.int32, scores.shape, 0)
        query_at = lax.broadcasted_iota(jnp.int32, scores.shape, 1) + causal_start
        scores = jnp.where(key_at <= query_at, scores, -jnp.inf)
    top = jnp.max(scores, axis=0, keepdims=True)
    weights = jnp.exp2((scores - top) * (scale * math.log2(math.e)))
    total = jnp.sum(weights, axis=0, keepdims=True)
    part = lax.dot_general(
        value, weights.astype(BF16), (((0,), (0,)), ((), ())), preferred_element_type=F32
    )
    return part / total, top * scale + jnp.log(total)


def plan_kernel(dims, picks, q, ask, slot, q_send, owner):
    n_seq, n_head, blocks, heads, n_pick, rows, width = dims
    pairs = blocks * heads
    me = lax.axis_index("seq")

    def find_owner(p):
        b, h = lax.div(p, heads), lax.rem(p, heads)
        found = [picks[b, h, t] for t in range(n_pick)]
        for t in range(n_pick):
            fresh = found[t] >= 0
            for earlier in range(t):
                fresh = fresh & (found[t] != found[earlier])
            owner[p * n_pick + t] = jnp.where(fresh, lax.div(found[t], blocks), -1)
            slot[p * n_pick + t] = -1

    loop(0, pairs, find_owner)

    def fill(s):
        def scan(p, carry):
            count, first, second = carry
            for t in range(n_pick):
                e = p * n_pick + t
                hit = owner[e] == s
                slot[e] = jnp.where(hit, s * CAP + count, slot[e])
                first = jnp.where(hit & (count == 0), e, first)
                second = jnp.where(hit & (count == 1), e, second)
                count = jnp.where(hit, count + 1, count)
            return count, first, second

        zero = jnp.int32(0)
        _, first, second = lax.fori_loop(0, pairs, scan, (zero, zero, zero))
        for c, e in enumerate((first, second)):
            p = lax.div(e, n_pick)
            pick = jnp.maximum(picks[lax.div(p, heads), lax.rem(p, heads), lax.rem(e, n_pick)], 0)
            ask[s, c] = lax.rem(pick, blocks) * heads + lax.rem(p, heads)
            q_send[s * CAP + c] = q[
                pl.ds(pl.multiple_of(lax.div(p, heads) * rows, rows), rows),
                pl.ds(pl.multiple_of(lax.rem(p, heads) * width, width), width),
            ]

    loop(0, me, fill)


def kernel(
    dims,
    q_hbm,
    k_hbm,
    v_hbm,
    ask,
    slot,
    q_send,
    w_hbm,
    out,
    q,
    k,
    v,
    w,
    asked,
    q_recv,
    o_send,
    o_recv,
    l_send,
    l_recv,
    own_o,
    own_l,
    gath,
    acc,
    load_sem,
    w_sem,
    ask_sem,
    qs_sem,
    os_sem,
    ls_sem,
    near_sem,
    cross_sem,
    fwd_sem,
):
    n_seq, n_head, blocks, heads, n_pick, rows, width = dims
    pairs = blocks * heads
    n_x = n_head // 2
    me = lax.axis_index("seq")
    hd = lax.axis_index("head")
    hx, hc = lax.div(hd, 2), lax.rem(hd, 2)
    mate = hx * 2 + 1 - hc

    def across(step):
        return lax.rem(hx + step, n_x) * 2 + hc

    def behind(step):
        return lax.rem(hx + n_x - step, n_x) * 2 + hc

    def load(i, p):
        src, dst = ((q_hbm, q), (k_hbm, k), (v_hbm, v))[i]
        b, h = lax.div(p, heads), lax.rem(p, heads)
        return pltpu.make_async_copy(
            src.at[
                pl.ds(pl.multiple_of(b * rows, rows), rows),
                pl.ds(pl.multiple_of(h * width, width), width),
            ],
            dst.at[p],
            load_sem.at[i, p],
        )

    def start_loads(p):
        for i in range(3):
            load(i, p).start()

    def end_loads(p):
        for i in range(3):
            load(i, p).wait()

    weight_load = pltpu.make_async_copy(w_hbm, w, w_sem.at[0])
    loop(0, pairs, start_loads)
    weight_load.start()

    barrier = pltpu.get_barrier_semaphore()

    def greet(d):
        pl.semaphore_signal(
            barrier, inc=1, device_id={"seq": lax.rem(me + d, n_seq)}, device_id_type=MESH
        )

    loop(1, n_seq, greet)
    for d in range(1, n_head):
        pl.semaphore_signal(
            barrier, inc=1, device_id={"head": lax.rem(hd + d, n_head)}, device_id_type=MESH
        )

    pl.semaphore_wait(barrier, n_seq + n_head - 2)

    def ask_copy(s, r):
        return pltpu.make_async_remote_copy(
            src_ref=ask.at[s],
            dst_ref=asked.at[r],
            send_sem=ask_sem.at[0, s],
            recv_sem=ask_sem.at[1, r],
            device_id={"seq": s},
            device_id_type=MESH,
        )

    def q_copy(s, r):
        return pltpu.make_async_remote_copy(
            src_ref=q_send.at[pl.ds(s * CAP, CAP)],
            dst_ref=q_recv.at[pl.ds(r * CAP, CAP)],
            send_sem=qs_sem.at[0, s],
            recv_sem=qs_sem.at[1, r],
            device_id={"seq": s},
            device_id_type=MESH,
        )

    def o_copy(r, s):
        return pltpu.make_async_remote_copy(
            src_ref=o_send.at[pl.ds(r * CAP, CAP)],
            dst_ref=o_recv.at[pl.ds(s * CAP, CAP)],
            send_sem=os_sem.at[0, r],
            recv_sem=os_sem.at[1, s],
            device_id={"seq": r},
            device_id_type=MESH,
        )

    def l_copy(r, s):
        return pltpu.make_async_remote_copy(
            src_ref=l_send.at[pl.ds(r * CAP, CAP)],
            dst_ref=l_recv.at[pl.ds(s * CAP, CAP)],
            send_sem=ls_sem.at[0, r],
            recv_sem=ls_sem.at[1, s],
            device_id={"seq": r},
            device_id_type=MESH,
        )

    def send_queries(s):
        ask_copy(s, me).start()
        q_copy(s, me).start()

    loop(0, me, send_queries)
    loop(0, pairs, end_loads)

    half = rows // 2

    def own(p):
        query, key, value = q[p], k[p], v[p]
        for part in range(2):
            seen = (part + 1) * half
            span = slice(part * half, seen)
            result, level = attend(query[span], key[:seen], value[:seen], part * half)
            own_o[p, :, span] = result
            own_l[p, :, span] = level

    def serve(r):
        ask_copy(me, r).wait_recv()
        q_copy(me, r).wait_recv()

        def one(c):
            code = asked[r, c]
            query, key, value = q_recv[r * CAP + c], k[code], v[code]
            for part in range(2):
                span = slice(part * half, (part + 1) * half)
                result, level = attend(query[span], key, value)
                o_send[r * CAP + c, :, span] = result.astype(BF16)
                l_send[r * CAP + c, :, span] = level

        loop(0, CAP, one)
        o_copy(r, me).start()
        l_copy(r, me).start()

    served = n_seq - 1 - me
    ahead = jnp.minimum(pairs, 4 * (me + 1))

    def round_of(t):
        lower = jnp.where(t == 0, 0, jnp.minimum(pairs, ahead + 2 * (t - 1)))
        upper = jnp.where(t == served, pairs, jnp.minimum(pairs, ahead + 2 * t))
        loop(lower, upper, own)

        @pl.when(t < served)
        def _():
            serve(n_seq - 1 - t)

    loop(0, served + 1, round_of)

    def collect(s):
        o_copy(s, s).wait_recv()
        l_copy(s, s).wait_recv()

    loop(0, me, collect)

    groups = heads // 2
    chunks = blocks * groups

    def head_copy(src, dst, sems, index, target):
        return pltpu.make_async_remote_copy(
            src_ref=gath.at[src, index],
            dst_ref=gath.at[dst, index],
            send_sem=sems[0],
            recv_sem=sems[1],
            device_id={"head": target},
            device_id_type=MESH,
        )

    def near_copy(index):
        return head_copy(hd, hd, (near_sem.at[0, index], near_sem.at[1, index]), index, mate)

    def cross_copy(step, index):
        sems = (cross_sem.at[0, step - 1, index], cross_sem.at[1, step - 1, index])
        return head_copy(hd, hd, sems, index, across(step))

    def fwd_copy(step, index):
        sems = (fwd_sem.at[0, step - 1, index], fwd_sem.at[1, step - 1, index])
        return head_copy(behind(step), behind(step), sems, index, mate)

    def merge(p):
        level = own_l[p]
        levels, slots = [], []
        for t in range(n_pick):
            at = slot[p * n_pick + t]
            safe = jnp.maximum(at, 0)
            far = l_recv[safe]
            levels.append(jnp.where(at >= 0, far, -jnp.inf))
            slots.append((at, safe))
        largest = level
        for far in levels:
            largest = jnp.maximum(largest, far)
        factor = jnp.exp(level - largest)
        denom = factor
        factors = []
        for far in levels:
            factors.append(jnp.exp(far - largest))
            denom = denom + factors[-1]
        numer = (factor / denom) * own_o[p]
        for (at, safe), far in zip(slots, factors):
            part = o_recv[safe].astype(F32)
            numer = numer + jnp.where(at >= 0, (far / denom) * part, 0.0)
        return numer.T.astype(BF16)

    def merge_group(index):
        for i in range(2):
            gath[hd, index, :, i * width : (i + 1) * width] = merge(index * 2 + i)
        for step in range(1, n_x):
            cross_copy(step, index).start()
        near_copy(index).start()

    loop(0, chunks, merge_group)
    weight_load.wait()

    depth = 2 * width

    def project(source, index, fresh=False):
        b, g = lax.div(index, groups), lax.rem(index, groups)
        at = pl.multiple_of((source * groups + g) * depth, depth)
        result = jnp.dot(
            gath[source, index], w[pl.ds(at, depth), :], preferred_element_type=F32
        )
        if fresh:
            acc[b] = result
        else:
            acc[b] += result

    def start_rows(b):
        acc[b] = jnp.zeros(acc.shape[1:], F32)

    loop(0, blocks, start_rows)
    loop(0, chunks, lambda index: project(hd, index))

    def take_near(index):
        near_copy(index).wait_recv()
        project(mate, index)

    loop(0, chunks, take_near)

    for step in range(1, n_x):

        def take_cross(index):
            cross_copy(step, index).wait_recv()
            fwd_copy(step, index).start()
            project(behind(step), index)
            fwd_copy(step, index).wait_recv()
            project(lax.rem(hx + n_x - step, n_x) * 2 + 1 - hc, index)

        loop(0, chunks, take_cross)

    def finish(b):
        out[pl.ds(pl.multiple_of(b * rows, rows), rows), :] = acc[b].astype(BF16)

    loop(0, blocks, finish)

    def sent_queries(s):
        ask_copy(s, me).wait_send()
        q_copy(s, me).wait_send()

    loop(0, me, sent_queries)

    def sent_results(r):
        o_copy(r, me).wait_send()
        l_copy(r, me).wait_send()

    loop(me + 1, n_seq, sent_results)

    def sent_heads(index):
        near_copy(index).wait_send()
        for step in range(1, n_x):
            cross_copy(step, index).wait_send()
            fwd_copy(step, index).wait_send()

    loop(0, chunks, sent_heads)


def solution(mesh):
    n_seq, n_head = mesh.shape["seq"], mesh.shape["head"]

    def body(query_rows, key_rows, value_rows, block_picks, out_weight):
        tok_rows, feature_width = query_rows.shape
        blocks, heads, n_pick = block_picks.shape
        rows, width = tok_rows // blocks, feature_width // heads
        pairs = blocks * heads
        chunks = pairs // 2
        n_x = n_head // 2
        any_spec = pl.BlockSpec(memory_space=pl.ANY)
        smem_spec = pl.BlockSpec(memory_space=pltpu.SMEM)
        vmem_spec = pl.BlockSpec(memory_space=pltpu.VMEM)
        out_width = out_weight.shape[1]
        slots = n_seq * CAP
        dma = pltpu.SemaphoreType.DMA
        dims = (n_seq, n_head, blocks, heads, n_pick, rows, width)
        ask, slot, q_send = pl.pallas_call(
            functools.partial(plan_kernel, dims),
            out_shape=(
                jax.ShapeDtypeStruct((n_seq, CAP), jnp.int32),
                jax.ShapeDtypeStruct((pairs * n_pick,), jnp.int32),
                jax.ShapeDtypeStruct((slots, rows, width), BF16),
            ),
            in_specs=[smem_spec, vmem_spec],
            out_specs=(smem_spec, smem_spec, vmem_spec),
            scratch_shapes=[pltpu.SMEM((pairs * n_pick,), jnp.int32)],
            name="plan",
        )(block_picks, query_rows)
        return pl.pallas_call(
            functools.partial(kernel, dims),
            out_shape=jax.ShapeDtypeStruct((tok_rows, out_width), BF16),
            in_specs=[any_spec] * 3 + [smem_spec] * 2 + [any_spec] * 2,
            out_specs=vmem_spec,
            scratch_shapes=[
                pltpu.VMEM((pairs, rows, width), BF16),
                pltpu.VMEM((pairs, rows, width), BF16),
                pltpu.VMEM((pairs, rows, width), BF16),
                pltpu.VMEM(out_weight.shape, BF16),
                pltpu.SMEM((n_seq, CAP), jnp.int32),
                pltpu.VMEM((slots, rows, width), BF16),
                pltpu.VMEM((slots, width, rows), BF16),
                pltpu.VMEM((slots, width, rows), BF16),
                pltpu.VMEM((slots, 1, rows), F32),
                pltpu.VMEM((slots, 1, rows), F32),
                pltpu.VMEM((pairs, width, rows), F32),
                pltpu.VMEM((pairs, 1, rows), F32),
                pltpu.VMEM((n_head, chunks, rows, 2 * width), BF16),
                pltpu.VMEM((blocks, rows, out_width), F32),
                dma((3, pairs)),
                dma((1,)),
                dma((2, n_seq)),
                dma((2, n_seq)),
                dma((2, n_seq)),
                dma((2, n_seq)),
                dma((2, chunks)),
                dma((2, max(n_x - 1, 1), chunks)),
                dma((2, max(n_x - 1, 1), chunks)),
            ],
            compiler_params=pltpu.CompilerParams(
                collective_id=0,
                has_side_effects=True,
                vmem_limit_bytes=67043328,
            ),
            name="layer",
        )(query_rows, key_rows, value_rows, ask, slot, q_send, out_weight)

    return jax.shard_map(
        body,
        mesh=mesh,
        in_specs=(
            P("seq", "head"),
            P("seq", "head"),
            P("seq", "head"),
            P("seq", "head", None),
            P(None, "head"),
        ),
        out_specs=P("seq", "head"),
        check_vma=False,
    )
```

```python
import functools
import math

import jax
import jax.numpy as jnp
from jax import lax
from jax.experimental import pallas as pl
from jax.experimental.pallas import tpu as pltpu
from jax.sharding import PartitionSpec as P

CAP = 2
MESH = pl.DeviceIdType.MESH
F32 = jnp.float32
BF16 = jnp.bfloat16


def loop(lower, upper, step):
    def body(i, carry):
        step(i)
        return carry

    lax.fori_loop(lower, upper, body, 0)


def attend(query, key, value, causal_start=None):
    scale = query.shape[-1] ** -0.5
    scores = lax.dot_general(
        key, query, (((1,), (1,)), ((), ())), preferred_element_type=F32
    )
    if causal_start is not None:
        key_at = lax.broadcasted_iota(jnp.int32, scores.shape, 0)
        query_at = lax.broadcasted_iota(jnp.int32, scores.shape, 1) + causal_start
        scores = jnp.where(key_at <= query_at, scores, -jnp.inf)
    top = jnp.max(scores, axis=0, keepdims=True)
    weights = jnp.exp2((scores - top) * (scale * math.log2(math.e)))
    total = jnp.sum(weights, axis=0, keepdims=True)
    part = lax.dot_general(
        value, weights.astype(BF16), (((0,), (0,)), ((), ())), preferred_element_type=F32
    )
    return part / total, top * scale + jnp.log(total)


def plan_kernel(dims, picks, q, ask, slot, q_send, owner):
    n_seq, n_head, blocks, heads, n_pick, rows, width = dims
    pairs = blocks * heads
    me = lax.axis_index("seq")

    def find_owner(p):
        b, h = lax.div(p, heads), lax.rem(p, heads)
        found = [picks[b, h, t] for t in range(n_pick)]
        for t in range(n_pick):
            fresh = found[t] >= 0
            for earlier in range(t):
                fresh = fresh & (found[t] != found[earlier])
            owner[p * n_pick + t] = jnp.where(fresh, lax.div(found[t], blocks), -1)
            slot[p * n_pick + t] = -1

    loop(0, pairs, find_owner)

    def fill(s):
        def scan(p, carry):
            count, first, second = carry
            for t in range(n_pick):
                e = p * n_pick + t
                hit = owner[e] == s
                slot[e] = jnp.where(hit, s * CAP + count, slot[e])
                first = jnp.where(hit & (count == 0), e, first)
                second = jnp.where(hit & (count == 1), e, second)
                count = jnp.where(hit, count + 1, count)
            return count, first, second

        zero = jnp.int32(0)
        _, first, second = lax.fori_loop(0, pairs, scan, (zero, zero, zero))
        for c, e in enumerate((first, second)):
            p = lax.div(e, n_pick)
            pick = jnp.maximum(picks[lax.div(p, heads), lax.rem(p, heads), lax.rem(e, n_pick)], 0)
            ask[s, c] = lax.rem(pick, blocks) * heads + lax.rem(p, heads)
            q_send[s * CAP + c] = q[
                pl.ds(pl.multiple_of(lax.div(p, heads) * rows, rows), rows),
                pl.ds(pl.multiple_of(lax.rem(p, heads) * width, width), width),
            ]

    loop(0, me, fill)


def kernel(
    dims,
    q_hbm,
    k_hbm,
    v_hbm,
    ask,
    slot,
    q_send,
    w_hbm,
    out,
    q,
    k,
    v,
    w,
    asked,
    q_recv,
    o_send,
    o_recv,
    l_send,
    l_recv,
    own_o,
    own_l,
    gath,
    acc,
    load_sem,
    w_sem,
    ask_sem,
    qs_sem,
    os_sem,
    ls_sem,
    near_sem,
    cross_sem,
    fwd_sem,
):
    n_seq, n_head, blocks, heads, n_pick, rows, width = dims
    pairs = blocks * heads
    n_x = n_head // 2
    me = lax.axis_index("seq")
    hd = lax.axis_index("head")
    hx, hc = lax.div(hd, 2), lax.rem(hd, 2)
    mate = hx * 2 + 1 - hc

    def across(step):
        return lax.rem(hx + step, n_x) * 2 + hc

    def behind(step):
        return lax.rem(hx + n_x - step, n_x) * 2 + hc

    def load(i, p):
        src, dst = ((q_hbm, q), (k_hbm, k), (v_hbm, v))[i]
        b, h = lax.div(p, heads), lax.rem(p, heads)
        return pltpu.make_async_copy(
            src.at[
                pl.ds(pl.multiple_of(b * rows, rows), rows),
                pl.ds(pl.multiple_of(h * width, width), width),
            ],
            dst.at[p],
            load_sem.at[i, p],
        )

    def start_loads(p):
        for i in range(3):
            load(i, p).start()

    def end_loads(p):
        for i in range(3):
            load(i, p).wait()

    weight_load = pltpu.make_async_copy(w_hbm, w, w_sem.at[0])
    loop(0, pairs, start_loads)
    weight_load.start()

    barrier = pltpu.get_barrier_semaphore()

    def greet(d):
        pl.semaphore_signal(
            barrier, inc=1, device_id={"seq": lax.rem(me + d, n_seq)}, device_id_type=MESH
        )

    loop(1, n_seq, greet)
    for d in range(1, n_head):
        pl.semaphore_signal(
            barrier, inc=1, device_id={"head": lax.rem(hd + d, n_head)}, device_id_type=MESH
        )

    pl.semaphore_wait(barrier, n_seq + n_head - 2)

    def ask_copy(s, r):
        return pltpu.make_async_remote_copy(
            src_ref=ask.at[s],
            dst_ref=asked.at[r],
            send_sem=ask_sem.at[0, s],
            recv_sem=ask_sem.at[1, r],
            device_id={"seq": s},
            device_id_type=MESH,
        )

    def q_copy(s, r):
        return pltpu.make_async_remote_copy(
            src_ref=q_send.at[pl.ds(s * CAP, CAP)],
            dst_ref=q_recv.at[pl.ds(r * CAP, CAP)],
            send_sem=qs_sem.at[0, s],
            recv_sem=qs_sem.at[1, r],
            device_id={"seq": s},
            device_id_type=MESH,
        )

    def o_copy(r, s):
        return pltpu.make_async_remote_copy(
            src_ref=o_send.at[pl.ds(r * CAP, CAP)],
            dst_ref=o_recv.at[pl.ds(s * CAP, CAP)],
            send_sem=os_sem.at[0, r],
            recv_sem=os_sem.at[1, s],
            device_id={"seq": r},
            device_id_type=MESH,
        )

    def l_copy(r, s):
        return pltpu.make_async_remote_copy(
            src_ref=l_send.at[pl.ds(r * CAP, CAP)],
            dst_ref=l_recv.at[pl.ds(s * CAP, CAP)],
            send_sem=ls_sem.at[0, r],
            recv_sem=ls_sem.at[1, s],
            device_id={"seq": r},
            device_id_type=MESH,
        )

    def send_queries(s):
        ask_copy(s, me).start()
        q_copy(s, me).start()

    loop(0, me, send_queries)
    loop(0, pairs, end_loads)

    half = rows // 2

    def own(p):
        query, key, value = q[p], k[p], v[p]
        for part in range(2):
            seen = (part + 1) * half
            span = slice(part * half, seen)
            result, level = attend(query[span], key[:seen], value[:seen], part * half)
            own_o[p, :, span] = result
            own_l[p, :, span] = level

    def serve(r):
        ask_copy(me, r).wait_recv()
        q_copy(me, r).wait_recv()

        def one(c):
            code = asked[r, c]
            query, key, value = q_recv[r * CAP + c], k[code], v[code]
            for part in range(2):
                span = slice(part * half, (part + 1) * half)
                result, level = attend(query[span], key, value)
                o_send[r * CAP + c, :, span] = result.astype(BF16)
                l_send[r * CAP + c, :, span] = level

        loop(0, CAP, one)
        o_copy(r, me).start()
        l_copy(r, me).start()

    served = n_seq - 1 - me
    ahead = jnp.minimum(pairs, 2 * me + 4)

    def round_of(t):
        lower = jnp.where(t == 0, 0, jnp.minimum(pairs, ahead + t - 1))
        upper = jnp.where(t == served, pairs, jnp.minimum(pairs, ahead + t))
        loop(lower, upper, own)

        @pl.when(t < served)
        def _():
            serve(n_seq - 1 - t)

    loop(0, served + 1, round_of)

    def collect(s):
        o_copy(s, s).wait_recv()
        l_copy(s, s).wait_recv()

    loop(0, me, collect)

    groups = heads // 2
    chunks = blocks * groups

    def head_copy(src, dst, sems, index, target):
        return pltpu.make_async_remote_copy(
            src_ref=gath.at[src, index],
            dst_ref=gath.at[dst, index],
            send_sem=sems[0],
            recv_sem=sems[1],
            device_id={"head": target},
            device_id_type=MESH,
        )

    def near_copy(index):
        return head_copy(hd, hd, (near_sem.at[0, index], near_sem.at[1, index]), index, mate)

    def cross_copy(step, index):
        sems = (cross_sem.at[0, step - 1, index], cross_sem.at[1, step - 1, index])
        return head_copy(hd, hd, sems, index, across(step))

    def fwd_copy(step, index):
        sems = (fwd_sem.at[0, step - 1, index], fwd_sem.at[1, step - 1, index])
        return head_copy(behind(step), behind(step), sems, index, mate)

    def merge(p):
        level = own_l[p]
        levels, slots = [], []
        for t in range(n_pick):
            at = slot[p * n_pick + t]
            safe = jnp.maximum(at, 0)
            far = l_recv[safe]
            levels.append(jnp.where(at >= 0, far, -jnp.inf))
            slots.append((at, safe))
        largest = level
        for far in levels:
            largest = jnp.maximum(largest, far)
        factor = jnp.exp(level - largest)
        denom = factor
        factors = []
        for far in levels:
            factors.append(jnp.exp(far - largest))
            denom = denom + factors[-1]
        numer = (factor / denom) * own_o[p]
        for (at, safe), far in zip(slots, factors):
            part = o_recv[safe].astype(F32)
            numer = numer + jnp.where(at >= 0, (far / denom) * part, 0.0)
        return numer.T.astype(BF16)

    def merge_group(index):
        for i in range(2):
            gath[hd, index, :, i * width : (i + 1) * width] = merge(index * 2 + i)
        for step in range(1, n_x):
            cross_copy(step, index).start()
        near_copy(index).start()

    loop(0, chunks, merge_group)
    weight_load.wait()

    depth = 2 * width

    def project(source, index, fresh=False):
        b, g = lax.div(index, groups), lax.rem(index, groups)
        at = pl.multiple_of((source * groups + g) * depth, depth)
        result = jnp.dot(
            gath[source, index], w[pl.ds(at, depth), :], preferred_element_type=F32
        )
        if fresh:
            acc[b] = result
        else:
            acc[b] += result

    def start_rows(b):
        acc[b] = jnp.zeros(acc.shape[1:], F32)

    loop(0, blocks, start_rows)
    loop(0, chunks, lambda index: project(hd, index))

    def take_near(index):
        near_copy(index).wait_recv()
        project(mate, index)

    loop(0, chunks, take_near)

    for step in range(1, n_x):

        def take_cross(index):
            cross_copy(step, index).wait_recv()
            fwd_copy(step, index).start()
            project(behind(step), index)
            fwd_copy(step, index).wait_recv()
            project(lax.rem(hx + n_x - step, n_x) * 2 + 1 - hc, index)

        loop(0, chunks, take_cross)

    def finish(b):
        out[pl.ds(pl.multiple_of(b * rows, rows), rows), :] = acc[b].astype(BF16)

    loop(0, blocks, finish)

    def sent_queries(s):
        ask_copy(s, me).wait_send()
        q_copy(s, me).wait_send()

    loop(0, me, sent_queries)

    def sent_results(r):
        o_copy(r, me).wait_send()
        l_copy(r, me).wait_send()

    loop(me + 1, n_seq, sent_results)

    def sent_heads(index):
        near_copy(index).wait_send()
        for step in range(1, n_x):
            cross_copy(step, index).wait_send()
            fwd_copy(step, index).wait_send()

    loop(0, chunks, sent_heads)


def solution(mesh):
    n_seq, n_head = mesh.shape["seq"], mesh.shape["head"]

    def body(query_rows, key_rows, value_rows, block_picks, out_weight):
        tok_rows, feature_width = query_rows.shape
        blocks, heads, n_pick = block_picks.shape
        rows, width = tok_rows // blocks, feature_width // heads
        pairs = blocks * heads
        chunks = pairs // 2
        n_x = n_head // 2
        any_spec = pl.BlockSpec(memory_space=pl.ANY)
        smem_spec = pl.BlockSpec(memory_space=pltpu.SMEM)
        vmem_spec = pl.BlockSpec(memory_space=pltpu.VMEM)
        out_width = out_weight.shape[1]
        slots = n_seq * CAP
        dma = pltpu.SemaphoreType.DMA
        dims = (n_seq, n_head, blocks, heads, n_pick, rows, width)
        ask, slot, q_send = pl.pallas_call(
            functools.partial(plan_kernel, dims),
            out_shape=(
                jax.ShapeDtypeStruct((n_seq, CAP), jnp.int32),
                jax.ShapeDtypeStruct((pairs * n_pick,), jnp.int32),
                jax.ShapeDtypeStruct((slots, rows, width), BF16),
            ),
            in_specs=[smem_spec, vmem_spec],
            out_specs=(smem_spec, smem_spec, vmem_spec),
            scratch_shapes=[pltpu.SMEM((pairs * n_pick,), jnp.int32)],
            name="plan",
        )(block_picks, query_rows)
        return pl.pallas_call(
            functools.partial(kernel, dims),
            out_shape=jax.ShapeDtypeStruct((tok_rows, out_width), BF16),
            in_specs=[any_spec] * 3 + [smem_spec] * 2 + [any_spec] * 2,
            out_specs=vmem_spec,
            scratch_shapes=[
                pltpu.VMEM((pairs, rows, width), BF16),
                pltpu.VMEM((pairs, rows, width), BF16),
                pltpu.VMEM((pairs, rows, width), BF16),
                pltpu.VMEM(out_weight.shape, BF16),
                pltpu.SMEM((n_seq, CAP), jnp.int32),
                pltpu.VMEM((slots, rows, width), BF16),
                pltpu.VMEM((slots, width, rows), BF16),
                pltpu.VMEM((slots, width, rows), BF16),
                pltpu.VMEM((slots, 1, rows), F32),
                pltpu.VMEM((slots, 1, rows), F32),
                pltpu.VMEM((pairs, width, rows), F32),
                pltpu.VMEM((pairs, 1, rows), F32),
                pltpu.VMEM((n_head, chunks, rows, 2 * width), BF16),
                pltpu.VMEM((blocks, rows, out_width), F32),
                dma((3, pairs)),
                dma((1,)),
                dma((2, n_seq)),
                dma((2, n_seq)),
                dma((2, n_seq)),
                dma((2, n_seq)),
                dma((2, chunks)),
                dma((2, max(n_x - 1, 1), chunks)),
                dma((2, max(n_x - 1, 1), chunks)),
            ],
            compiler_params=pltpu.CompilerParams(
                collective_id=0,
                has_side_effects=True,
                vmem_limit_bytes=67043328,
            ),
            name="layer",
        )(query_rows, key_rows, value_rows, ask, slot, q_send, out_weight)

    return jax.shard_map(
        body,
        mesh=mesh,
        in_specs=(
            P("seq", "head"),
            P("seq", "head"),
            P("seq", "head"),
            P("seq", "head", None),
            P(None, "head"),
        ),
        out_specs=P("seq", "head"),
        check_vma=False,
    )
```
